32 devices in a mesh: row: 4 (over x, core), col: 8 (over z, y).
Axes of the slice: x: 2, y: 2, z: 4, core: 2. Of those that a mesh axis runs over, the one named last changes fastest.
Arguments:
- rhs_c: float32 [12, 512, 6, 1024], P(None, 'row', None, 'col'), may hold values from -6 to 6
- rhs_f: float32 [12, 512, 6, 1024], P(None, 'row', None, 'col'), may hold values from -6 to 6
- pencil_a: bfloat16 [12, 512, 6, 1024], P(None, 'row', None, 'col'), may hold values from -0.5 to 0.5
- pencil_d: bfloat16 [12, 512, 6, 1024], P(None, 'row', None, 'col'), may hold values from -0.5 to 0.5
- pencil_b: bfloat16 [12, 512, 6, 1024], P(None, 'row', None, 'col'), may hold values from -0.5 to 0.5
- pencil_e: bfloat16 [12, 512, 6, 1024], P(None, 'row', None, 'col'), may hold values from -0.5 to 0.5
- d_inverse: float32 [12, 512, 128], P(None, 'row'), may hold values from -0.25 to 2.5
- left_vectors: float32 [12, 512, 128], P(None, 'row'), may hold values from -0.25 to 2.5
- left_inverse: float32 [12, 512, 128], P(None, 'row'), may hold values from -0.25 to 2.5
- left_eigs: float32 [12, 512], P(None, 'row'), may hold values from 1 to 3
- e_inverse: float32 [6, 1024, 128], P(None, 'col'), may hold values from -0.25 to 2.5
- right_vectors: float32 [6, 1024, 128], P(None, 'col'), may hold values from -0.25 to 2.5
- right_inverse: float32 [6, 1024, 128], P(None, 'col'), may hold values from -0.25 to 2.5
- right_eigs: float32 [6, 1024], P(None, 'col'), may hold values from -3 to -1
Outputs:
- updated_c: float32 [12, 512, 6, 1024], P(None, 'row', None, 'col')
- updated_f: float32 [12, 512, 6, 1024], P(None, 'row', None, 'col')
- solved_r: float32 [12, 512, 6, 1024], P(None, 'row', None, 'col')
- solved_l: float32 [12, 512, 6, 1024], P(None, 'row', None, 'col')
The draws below stay inside these ranges and needn't reach their ends.
All inputs are finite; a program needn't handle non-finite values.
Results may differ from the reference program's by a relative error of at most 0.0003.
Values may be sent and summed in bfloat16 or wider, within the bound.
A program may use at most 128 MiB of HBM per device.

```python
import math
import jax
import jax.numpy as jnp
from jax import lax

TILE = 128
ORDER = 6144
STEPS = 3
RT = 12
CT = 6
N_ROW = 4
N_COL = 8


def dominant(key, lead, height, salt):
    key = jax.random.fold_in(key, salt)
    first, second = jax.random.split(key)
    shape = (lead, height, TILE)
    diagonal = jnp.exp(jax.random.uniform(first, shape, jnp.float32, 0.0, math.log(2.0)))
    spread = jnp.clip(0.4 / math.sqrt(TILE) * jax.random.normal(second, shape, jnp.float32), -0.25, 0.25)
    rows = lax.broadcasted_iota(jnp.int32, shape, 1) % TILE
    cols = lax.broadcasted_iota(jnp.int32, shape, 2)
    return jnp.where(rows == cols, diagonal, spread)


def draw_d_inverse(key, part):
    return dominant(key, RT, N_ROW * TILE, 11)


def draw_left_vectors(key, part):
    return dominant(key, RT, N_ROW * TILE, 12)


def draw_left_inverse(key, part):
    return dominant(key, RT, N_ROW * TILE, 13)


def draw_e_inverse(key, part):
    return dominant(key, CT, N_COL * TILE, 14)


def draw_right_vectors(key, part):
    return dominant(key, CT, N_COL * TILE, 15)


def draw_right_inverse(key, part):
    return dominant(key, CT, N_COL * TILE, 16)


def levels(stream_key, dims, shards, low, top_value):
    def one(dim, blocks):
        steps = jax.random.uniform(jax.random.fold_in(jax.random.fold_in(stream_key, 6), dim), (blocks,), jnp.float32, low / len(shards), top_value / len(shards))
        return jnp.repeat(jnp.exp(steps), dims[dim] // blocks).reshape((-1,) + (1,) * (len(dims) - dim - 1))

    factor_of = one(*shards[0])
    for cut in shards[1:]:
        factor_of = factor_of * one(*cut)
    return factor_of


def scatter_about(key, extent, width, limit, cuts=(), kind=jnp.bfloat16):
    entries = width * jax.random.normal(key, extent, jnp.float32)
    if cuts:
        entries = entries * levels(key, extent, cuts, -0.22, 0.18)
    return jnp.clip(entries, -limit, limit).astype(kind)


def setup_inputs(seed: int = 0) -> dict:
    seeds = jax.random.split(jax.random.key(seed), 15)
    return {
        "rhs_c": scatter_about(seeds[0], (RT, N_ROW * TILE, CT, N_COL * TILE), 1.0, 6.0, ((1, 4), (3, 8)), jnp.float32),
        "rhs_f": scatter_about(seeds[1], (RT, N_ROW * TILE, CT, N_COL * TILE), 1.0, 6.0, ((1, 4), (3, 8)), jnp.float32),
        "pencil_a": scatter_about(seeds[2], (RT, N_ROW * TILE, CT, N_COL * TILE), TILE ** -0.5, 0.5, ((1, 4), (3, 8))),
        "pencil_d": scatter_about(seeds[3], (RT, N_ROW * TILE, CT, N_COL * TILE), TILE ** -0.5, 0.5, ((1, 4), (3, 8))),
        "pencil_b": scatter_about(seeds[4], (RT, N_ROW * TILE, CT, N_COL * TILE), TILE ** -0.5, 0.5, ((1, 4), (3, 8))),
        "pencil_e": scatter_about(seeds[5], (RT, N_ROW * TILE, CT, N_COL * TILE), TILE ** -0.5, 0.5, ((1, 4), (3, 8))),
        "d_inverse": draw_d_inverse(jax.random.fold_in(seeds[14], 71), 0),
        "left_vectors": draw_left_vectors(jax.random.fold_in(seeds[14], 71), 0),
        "left_inverse": draw_left_inverse(jax.random.fold_in(seeds[14], 71), 0),
        "left_eigs": jnp.clip(jnp.exp(math.log(3.0) - 1.0986123 * jax.random.uniform(seeds[9], (RT, N_ROW * TILE), jnp.float32) ** levels(seeds[9], (RT, N_ROW * TILE), ((1, 4),), -0.2, 0.2)), 1.0, 3.0),
        "e_inverse": draw_e_inverse(jax.random.fold_in(seeds[14], 71), 0),
        "right_vectors": draw_right_vectors(jax.random.fold_in(seeds[14], 71), 0),
        "right_inverse": draw_right_inverse(jax.random.fold_in(seeds[14], 71), 0),
        "right_eigs": jnp.clip(-3.0 + 2.0 * jax.random.uniform(seeds[13], (CT, N_COL * TILE), jnp.float32) ** levels(seeds[13], (CT, N_COL * TILE), ((1, 8),), -0.2, 0.2), -3.0, -1.0),
    }


def product(left, right):
    return jnp.einsum("bij,bjk->bik", left, right, precision=lax.Precision.HIGHEST)


def solve_tiles(a_diag, e_diag, resid_c, resid_f, inv_d, vec_left, back_left, eig_left, inv_e, vec_right, back_right, eig_right):
    coupled = product(a_diag, inv_d)
    merged = product(resid_c - product(coupled, resid_f), inv_e)
    spectral = product(product(back_left, merged), vec_right)
    spectral = spectral / (eig_left[:, :, None] - eig_right[:, None, :])
    new_l = product(product(vec_left, spectral), back_right)
    new_r = product(inv_d, resid_f + product(new_l, e_diag))
    return new_r, new_l


def reference(rhs_c, rhs_f, pencil_a, pencil_d, pencil_b, pencil_e, d_inverse, left_vectors, left_inverse, left_eigs, e_inverse, right_vectors, right_inverse, right_eigs):
    blocks = ORDER // TILE
    highest = lax.Precision.HIGHEST

    def grid(field):
        return field.astype(jnp.float32).reshape(blocks, TILE, blocks, TILE)

    current_c = grid(rhs_c)
    current_f = grid(rhs_f)
    tiles_a = grid(pencil_a)
    tiles_d = grid(pencil_d)
    tiles_b = grid(pencil_b)
    tiles_e = grid(pencil_e)
    inv_d = d_inverse.reshape(blocks, TILE, TILE)
    vec_left = left_vectors.reshape(blocks, TILE, TILE)
    back_left = left_inverse.reshape(blocks, TILE, TILE)
    eig_left = left_eigs.reshape(blocks, TILE)
    inv_e = e_inverse.reshape(blocks, TILE, TILE)
    vec_right = right_vectors.reshape(blocks, TILE, TILE)
    back_right = right_inverse.reshape(blocks, TILE, TILE)
    eig_right = right_eigs.reshape(blocks, TILE)
    out_r = jnp.zeros_like(current_c)
    out_l = jnp.zeros_like(current_c)
    count = jnp.arange(blocks, dtype=jnp.int32)
    for step in range(STEPS):
        offset = 1 - step
        front_rows = count + offset
        col_valid = (front_rows >= 0) & (front_rows < blocks)
        rows_clip = jnp.clip(front_rows, 0, blocks - 1).astype(jnp.int32)
        front_cols = count - offset
        row_valid = (front_cols >= 0) & (front_cols < blocks)
        cols_clip = jnp.clip(front_cols, 0, blocks - 1).astype(jnp.int32)
        resid_c = current_c[rows_clip, :, count, :]
        resid_f = current_f[rows_clip, :, count, :]
        a_diag = tiles_a[rows_clip, :, rows_clip, :]
        e_diag = tiles_e[count, :, count, :]
        new_r, new_l = solve_tiles(a_diag, e_diag, resid_c, resid_f, inv_d[rows_clip], vec_left[rows_clip], back_left[rows_clip], eig_left[rows_clip], inv_e, vec_right, back_right, eig_right)
        new_r = jnp.where(col_valid[:, None, None], new_r, 0.0)
        new_l = jnp.where(col_valid[:, None, None], new_l, 0.0)
        panel_a = tiles_a[:, :, rows_clip, :]
        panel_d = tiles_d[:, :, rows_clip, :]
        mask_a = (count[:, None] < front_rows[None, :]) & col_valid[None, :]
        term_c = jnp.einsum("kpjq,jqs->kpjs", panel_a, new_r, precision=highest)
        term_f = jnp.einsum("kpjq,jqs->kpjs", panel_d, new_r, precision=highest)
        row_l = jnp.where(row_valid[:, None, None], new_l[cols_clip], 0.0)
        panel_b = tiles_b[cols_clip]
        panel_e = tiles_e[cols_clip]
        mask_b = (count[None, :] > front_cols[:, None]) & row_valid[:, None]
        gain_c = jnp.einsum("ipq,iqls->ipls", row_l, panel_b, precision=highest)
        gain_f = jnp.einsum("ipq,iqls->ipls", row_l, panel_e, precision=highest)
        wide_a = mask_a[:, None, :, None]
        wide_b = mask_b[:, None, :, None]
        current_c = current_c - jnp.where(wide_a, term_c, 0.0) + jnp.where(wide_b, gain_c, 0.0)
        current_f = current_f - jnp.where(wide_a, term_f, 0.0) + jnp.where(wide_b, gain_f, 0.0)
        out_r = out_r.at[rows_clip, :, count, :].add(new_r)
        out_l = out_l.at[rows_clip, :, count, :].add(new_l)
    shape = (RT, N_ROW * TILE, CT, N_COL * TILE)
    return current_c.reshape(shape), current_f.reshape(shape), out_r.reshape(shape), out_l.reshape(shape)
```

```python
import functools

import jax
import jax.numpy as jnp
from jax import lax
from jax.experimental import pallas as pl
from jax.experimental.pallas import tpu as pltpu
from jax.sharding import PartitionSpec as P

TILE = 128
PIECES = 3


def product(left, right):
    return jnp.einsum("bij,bjk->bik", left, right, precision=lax.Precision.HIGHEST)


def half_product(exact, value):
    hi, lo = split(value)
    dot = functools.partial(jnp.einsum, "bij,bjk->bik", preferred_element_type=jnp.float32)
    return dot(exact, hi) + dot(exact, lo)


def product_half(value, exact):
    hi, lo = split(value)
    dot = functools.partial(jnp.einsum, "bij,bjk->bik", preferred_element_type=jnp.float32)
    return dot(hi, exact) + dot(lo, exact)


def split(value):
    hi = lax.reduce_precision(value, 8, 7)
    return hi.astype(jnp.bfloat16), (value - hi).astype(jnp.bfloat16)


def heights(rows_dev, cols_dev, count_rows, count_cols):
    return [min(rows_dev, (b * count_cols + count_cols - 1) // count_rows + 1) for b in range(cols_dev)]


def pack(left, right, tall):
    tiles = [jnp.stack([left[:n, b], right[:n, b]]) for b, n in enumerate(tall)]
    return jnp.concatenate(tiles, axis=1)


def update_kernel(
    count_rows, count_cols, place, c_ref, f_ref, a_ref, d_ref, b_ref, e_ref, r_ref, l_ref, ad_ref, be_ref, c_out, f_out
):
    a = pl.program_id(0)
    row, col = place[0], place[1]
    cols_dev = c_ref.shape[1]
    total = ad_ref.shape[2]
    i = a * count_rows + row
    col_side, row_side = lax.rem(col, 2), lax.rem(row, 2)
    for b in range(cols_dev):
        j = b * count_cols + col

        @pl.when(i > j)
        def _():
            c_out[0, b] = c_ref[0, b]
            f_out[0, b] = f_ref[0, b]

        @pl.when(i <= j)
        def _():
            slot_right = jnp.minimum(b + (col == count_cols - 1).astype(jnp.int32), cols_dev - 1)
            slot_left = jnp.maximum(b - (col == 0).astype(jnp.int32), 0)
            right = jnp.clip(place[2 + slot_right] + a, 0, total - 1)
            left = jnp.clip(place[2 + slot_left] + a, 0, total - 1)
            up = jnp.clip(place[2 + b] + a - (row == 0).astype(jnp.int32), 0, total - 1)
            down = jnp.clip(place[2 + b] + a + (row == count_rows - 1).astype(jnp.int32), 0, total - 1)
            keep_mid = jnp.full((TILE, TILE), jnp.where(i < j, 1.0, 0.0), jnp.float32).astype(jnp.bfloat16)
            keep_far = jnp.full((TILE, TILE), jnp.where(i < j - 1, 1.0, 0.0), jnp.float32).astype(jnp.bfloat16)

            def wide(which, own):
                return jnp.concatenate(
                    [ad_ref[col_side, which, right], own * keep_mid, ad_ref[1 - col_side, which, left] * keep_far], axis=1
                )

            lhs = jnp.concatenate([wide(0, a_ref[0, b]), wide(1, d_ref[0, b])], axis=0)
            first = jnp.dot(lhs, r_ref[b], preferred_element_type=jnp.float32)

            def tall(which, own):
                return jnp.concatenate(
                    [be_ref[1 - row_side, which, up], own * keep_mid, be_ref[row_side, which, down] * keep_far], axis=0
                )

            rhs = jnp.concatenate([tall(0, b_ref[0, b]), tall(1, e_ref[0, b])], axis=1)
            second = jnp.dot(l_ref[0], rhs, preferred_element_type=jnp.float32)
            c_out[0, b] = (
                c_ref[0, b]
                - (first[:TILE, :TILE] + first[:TILE, TILE:])
                + (second[:TILE, :TILE] + second[TILE:, :TILE])
            )
            f_out[0, b] = (
                f_ref[0, b]
                - (first[TILE:, :TILE] + first[TILE:, TILE:])
                + (second[:TILE, TILE:] + second[TILE:, TILE:])
            )


def body(
    rhs_c,
    rhs_f,
    pencil_a,
    pencil_d,
    pencil_b,
    pencil_e,
    d_inverse,
    left_vectors,
    left_inverse,
    left_eigs,
    e_inverse,
    right_vectors,
    right_inverse,
    right_eigs,
):
    count_rows = lax.axis_size("row")
    count_cols = lax.axis_size("col")
    row = lax.axis_index("row")
    col = lax.axis_index("col")
    c, f, a, d, b, e = [
        x.transpose(0, 2, 1, 3) for x in (rhs_c, rhs_f, pencil_a, pencil_d, pencil_b, pencil_e)
    ]
    rows_dev, cols_dev = c.shape[:2]
    blocks = rows_dev * count_rows
    slots = jnp.arange(cols_dev, dtype=jnp.int32)
    block_cols = slots * count_cols + col
    tall = heights(rows_dev, cols_dev, count_rows, count_cols)
    offsets = [sum(tall[:k]) for k in range(cols_dev)]

    def shift(value, axis, by):
        n = lax.axis_size(axis)
        return lax.ppermute(value, axis, [(k, (k + by) % n) for k in range(n)])

    band = jnp.clip((block_cols - row) // count_rows, 0, rows_dev - 1)
    band_ad = jnp.stack([a[band, slots], d[band, slots]])
    band_be = jnp.stack([b[band, slots], e[band, slots]])
    from_right = shift(band_ad, "col", -1)
    from_left = shift(band_ad[0], "col", 1)
    from_up = shift(band_be, "row", 1)
    from_down = shift(band_be[1], "row", -1)
    from_right = jnp.where(col == count_cols - 1, jnp.roll(from_right, -1, axis=1), from_right)
    from_left = jnp.where(col == 0, jnp.roll(from_left, 1, axis=0), from_left)

    pack_ad = pack(a, d, tall)
    pack_be = pack(b, e, tall)
    total = pack_ad.shape[1]
    pieces = min(PIECES, total)
    cuts = [total * k // pieces for k in range(pieces + 1)]
    swap_col = [(k, k ^ 1) for k in range(count_cols)]
    relay_col = [(k, (k + 2 if k % 2 == 0 else k - 2) % count_cols) for k in range(count_cols)]
    swap_row = [(k, k ^ 1) for k in range(count_rows)]
    cross_row = [(k, (k - 1 if k % 2 == 0 else k + 1) % count_rows) for k in range(count_rows)]
    swapped, relayed = [], []
    for lo, hi in zip(cuts[:-1], cuts[1:]):
        got = lax.ppermute(pack_ad[:, lo:hi], "col", swap_col)
        swapped.append(got)
        relayed.append(lax.ppermute(got, "col", relay_col))
    be_swap = lax.ppermute(pack_be, "row", swap_row)
    be_cross = lax.ppermute(pack_be, "row", cross_row)
    near_ad = jnp.stack([jnp.concatenate(swapped, axis=1), jnp.concatenate(relayed, axis=1)])
    near_be = jnp.stack([be_swap, be_cross])

    phase = (col - row) % count_rows
    ahead = phase == count_rows - 1
    level = phase == 0
    behind = phase == 1
    mine = (block_cols + 1 - row) // count_rows
    front_rows = mine * count_rows + row
    valid = (ahead | level | behind) & (front_rows >= 0) & (front_rows < blocks)
    mine = jnp.clip(mine, 0, rows_dev - 1)
    front_c = c[mine, slots]
    front_f = f[mine, slots]
    own_a, own_d, own_b, own_e = [x[mine, slots] for x in (a, d, b, e)]
    a_diag = jnp.where(ahead, from_right[0], jnp.where(level, own_a, from_left)).astype(jnp.float32)
    e_diag = jnp.where(ahead, from_up[1], jnp.where(level, own_e, from_down)).astype(jnp.float32)
    inv_d, vec_left, back_left = d_inverse[mine], left_vectors[mine], left_inverse[mine]
    spread = left_eigs[mine][:, :, None] - right_eigs[:, None, :]
    coupled = product(a_diag, inv_d)

    def solve(resid_c, resid_f):
        merged = product(resid_c - product(coupled, resid_f), e_inverse)
        spectral = product(product(back_left, merged), right_vectors) / spread
        new_l = product(product(vec_left, spectral), right_inverse)
        new_r = product(inv_d, resid_f + product(new_l, e_diag))
        keep = valid[:, None, None]
        return jnp.where(keep, new_r, 0.0), jnp.where(keep, new_l, 0.0)

    def onward(value, by):
        got = shift(value, "col", by)
        moved = jnp.concatenate([jnp.zeros_like(got[:1]), got[:-1]])
        return jnp.where(col < by, moved, got)

    r_one, l_one = solve(front_c, front_f)
    r_in, l_in = shift(r_one, "row", -1), onward(l_one, 1)
    r_far, l_far = shift(r_one, "row", -2), onward(l_one, 2)
    r_two, l_two = solve(
        front_c - half_product(from_right[0], r_in) + product_half(l_in, from_up[0]),
        front_f - half_product(from_right[1], r_in) + product_half(l_in, from_up[1]),
    )
    base_c = front_c - half_product(from_right[0], r_far) + product_half(l_far, from_up[0])
    base_f = front_f - half_product(from_right[1], r_far) + product_half(l_far, from_up[1])
    r_in, l_in = shift(r_two, "row", -1), onward(l_two, 1)
    r_three, l_three = solve(
        base_c - half_product(own_a, r_in) + product_half(l_in, own_b),
        base_f - half_product(own_d, r_in) + product_half(l_in, own_e),
    )
    new_r = jnp.where(ahead, r_one, jnp.where(level, r_two, r_three))
    new_l = jnp.where(ahead, l_one, jnp.where(level, l_two, l_three))

    every_r = lax.all_gather(new_r, "row")
    every_l = lax.all_gather(new_l, "col")
    r_parts, l_parts = [], []
    block_rows = jnp.arange(rows_dev, dtype=jnp.int32) * count_rows + row
    for offset in (1, 0, -1):
        r_parts.append(every_r[(col + offset) % count_rows])
        at = block_rows - offset
        inside = (at >= 0) & (at < blocks)
        at = jnp.clip(at, 0, blocks - 1)
        l_parts.append(jnp.where(inside[:, None, None], every_l[at % count_cols, at // count_cols], 0.0))
    r_all = jnp.concatenate(split(jnp.concatenate(r_parts, axis=1)), axis=2)
    l_all = jnp.concatenate(split(jnp.concatenate(l_parts, axis=2)), axis=1)

    place = jnp.concatenate([jnp.stack([row, col]).astype(jnp.int32), jnp.array(offsets, jnp.int32)])
    line = pl.BlockSpec((1, cols_dev, TILE, TILE), lambda k: (k, 0, 0, 0))
    whole = pl.BlockSpec(memory_space=pltpu.VMEM)
    new_c, new_f = pl.pallas_call(
        functools.partial(update_kernel, count_rows, count_cols),
        grid=(rows_dev,),
        in_specs=[pl.BlockSpec(memory_space=pltpu.SMEM)]
        + [line] * 6
        + [whole, pl.BlockSpec((1, 2 * TILE, 3 * TILE), lambda k: (k, 0, 0)), whole, whole],
        out_specs=[line, line],
        out_shape=[jax.ShapeDtypeStruct(c.shape, jnp.float32)] * 2,
        compiler_params=pltpu.CompilerParams(vmem_limit_bytes=48 * 1024 * 1024),
        name="update",
    )(place, c, f, a, d, b, e, r_all, l_all, near_ad, near_be)

    here = (valid[None, :] & (jnp.arange(rows_dev, dtype=jnp.int32)[:, None] == mine[None, :]))[:, :, None, None]
    out_r = jnp.where(here, new_r[None], 0.0)
    out_l = jnp.where(here, new_l[None], 0.0)
    return tuple(x.transpose(0, 2, 1, 3) for x in (new_c, new_f, out_r, out_l))


def solution(mesh):
    grid = P(None, "row", None, "col")
    left, right = P(None, "row", None), P(None, "col", None)
    in_specs = (grid,) * 6 + (left,) * 3 + (P(None, "row"),) + (right,) * 3 + (P(None, "col"),)
    return jax.shard_map(body, mesh=mesh, in_specs=in_specs, out_specs=(grid,) * 4, check_vma=False)
```
